32 devices in a mesh: parts: 2 (over y), rows: 4 (over x, core), cols: 4 (over z).
Axes of the slice: x: 2, y: 2, z: 4, core: 2. Of those that a mesh axis runs over, the one named last changes fastest.
Arguments:
- singles: bfloat16 [1024, 384], P(('parts', 'rows', 'cols')), parts along dimension 0, may hold values from -120 to 120
- pair: bfloat16 [1024, 512, 128], P(('parts', 'rows'), 'cols'), parts along dimension 0, may hold values from -6 to 6
- chain_sizes: int32 [16], P('parts'), parts along dimension 0, may hold values from 1 to 128, 512 in all
- single_proj: bfloat16 [384, 1536], replicated, may hold values from -1 to 1
- query_bias: float32 [384], replicated, may hold values from -5 to 5
- pair_proj: bfloat16 [128, 16], replicated, may hold values from -0.5 to 0.5
- out_proj: bfloat16 [384, 384], replicated, may hold values from -1.25 to 1.25
Outputs:
- update: bfloat16 [1024, 384], P(('parts', 'rows', 'cols')), parts along dimension 0
The draws below stay inside these ranges and needn't reach their ends.
There are 2 independent parts, one for each index of `parts`. The reference program is written for one: setup_inputs(seed, part) draws one part's arguments, and reference() takes and returns one part's arrays. A program takes and returns all parts, laid end to end along the dimension named above; an argument that names none is the same for every part. Nothing has to cross between parts.
Inputs may be any that keep to these rules, and one draw needn't show every extreme that they name: `chain_sizes`: the first 7 entries count the tokens of the chains in order; the last one counts the padding tokens at the end of the complex.
All inputs are finite; a program needn't handle non-finite values.
Results may differ from the reference program's by a relative error of at most 0.004.
The reference program's roundings to bfloat16 on the way (of `normed`, `queries`, `pair_normed`, `pair_bias`, `rounded` and `attended`) count: a program that leaves them out, or rounds other values in their place, can miss the bound.
Values may be sent and summed in bfloat16 or wider, within the bound.
A program may use at most 64 MiB of HBM per device.

```python
import math
import jax
import jax.numpy as jnp
import numpy as np
from jax import lax

C = 384
CZ = 128
H = 16
SLOTS = 8
TOKENS = 512


def draw_singles(key, part):
    noise = jnp.clip(jax.random.normal(key, (TOKENS, C), jnp.float32), -6.0, 6.0)
    return noise.astype(jnp.bfloat16)


def draw_single_proj(key, part):
    base = jnp.clip(jax.random.normal(key, (C, 4 * C), jnp.float32), -4.0, 4.0) / math.sqrt(C)
    return base.astype(jnp.bfloat16)


def shard_levels(key, shape, pieces, low, largest):
    def one(axis_at, parts):
        steps = jax.random.uniform(jax.random.fold_in(jax.random.fold_in(key, 6), axis_at), (parts,), jnp.float32, low / len(pieces), largest / len(pieces))
        return jnp.repeat(jnp.exp(steps), shape[axis_at] // parts).reshape((-1,) + (1,) * (len(shape) - axis_at - 1))

    gain = one(*pieces[0])
    for cut in pieces[1:]:
        gain = gain * one(*cut)
    return gain


def profile(number_of, total, reach, lean):
    portions = [(1 << 20) // math.isqrt(grade ** lean) + 1 for grade in range(2, number_of + 1)]
    spare, given = total - reach - (number_of - 1), [1] * (number_of - 1)
    while spare > 0:
        free = [i for i in range(number_of - 1) if given[i] < reach]
        whole, left = sum([portions[i] for i in free]), spare
        for i in free:
            more = min(reach - given[i], max(1, left * portions[i] // whole), spare)
            given[i] = given[i] + more
            spare = spare - more
    return np.array([reach] + given)


def uneven(stream_key, count, total, reach, slope):
    if count == 2:
        one = jax.random.randint(stream_key, (), max(1, total - reach), min(reach, total - 1) + 1)
        return jnp.stack([one, total - one])
    lengths = jnp.asarray(profile(count, total, reach, slope), jnp.int32)
    twos = (count - 1) // 2
    donor, sink = lengths[1:1 + 2 * twos:2], lengths[2:2 + 2 * twos:2]
    room = jnp.minimum(donor - 1, reach - sink)
    moved = jax.random.randint(jax.random.fold_in(stream_key, 1), (twos,), 0, 1 << 20) % (room + 1)
    lengths = lengths.at[1:1 + 2 * twos:2].set(donor - moved).at[2:2 + 2 * twos:2].set(sink + moved)
    return lengths[jax.random.permutation(jax.random.fold_in(stream_key, 2), count)]


def centred(stream_key, extent, spread, limit, cuts=(), kind=jnp.bfloat16):
    factor_of = shard_levels(stream_key, extent, cuts, -0.22, 0.18) if cuts else 1.0
    entries = jax.random.normal(stream_key, extent, jnp.float32) * spread * factor_of
    return jnp.minimum(jnp.maximum(entries, -limit), limit).astype(kind)


def setup_inputs(seed: int = 0, part: int = 0) -> dict:
    key_of = jax.random.split(jax.random.key(seed), 8)
    own_keys = jax.random.split(jax.random.fold_in(key_of[7], part), 8)
    singles = draw_singles(jax.random.fold_in(jax.random.fold_in(key_of[7], part), 71), part)
    pair = centred(own_keys[1], (TOKENS, TOKENS, CZ), 1.0, 6.0, ((0, 4), (1, 4)))
    chain_sizes = uneven(own_keys[2], SLOTS, TOKENS, TOKENS // 4, 1).astype(jnp.int32)
    single_proj = draw_single_proj(jax.random.fold_in(key_of[7], 71), part)
    query_bias = centred(key_of[4], (C,), 1.0, 5.0, (), jnp.float32)
    pair_proj = centred(key_of[5], (CZ, H), CZ ** -0.5, 0.5)
    out_proj = centred(key_of[6], (C, C), (C // 16) ** -0.5, 1.25)
    return dict(singles=singles, pair=pair, chain_sizes=chain_sizes, single_proj=single_proj, query_bias=query_bias, pair_proj=pair_proj, out_proj=out_proj)


def normalize(matrix):
    average = lax.optimization_barrier(jnp.mean(matrix, axis=-1, keepdims=True))
    centered = matrix - average
    variance = lax.optimization_barrier(jnp.mean(centered * centered, axis=-1, keepdims=True))
    return centered * lax.rsqrt(variance + 1e-05)

def reference(singles, pair, chain_sizes, single_proj, query_bias, pair_proj, out_proj):
    features = C
    head_dim = C // H
    score_scale = head_dim ** (-0.5)
    normed = normalize(singles.astype(jnp.float32)).astype(jnp.bfloat16)
    projected = jnp.dot(normed, single_proj, preferred_element_type=jnp.float32)
    queries = (projected[:, :features] + query_bias.astype(jnp.float32)).astype(jnp.bfloat16)
    key_rows = projected[:, features:2 * features].astype(jnp.bfloat16)
    values = projected[:, 2 * features:3 * features].astype(jnp.bfloat16)
    gating = jax.nn.sigmoid(projected[:, 3 * features:])
    live_count = jnp.sum(chain_sizes[:-1])
    key_live = jnp.arange(TOKENS, dtype=jnp.int32) < live_count
    key_heads = key_rows.astype(jnp.float32).reshape(TOKENS, H, head_dim)
    value_heads = values.astype(jnp.float32).reshape(TOKENS, H, head_dim)
    row_block = min(TOKENS, 128)
    block_count = TOKENS // row_block

    def one_block(block_index):
        first_row = (block_index * row_block).astype(jnp.int32)
        pair_rows = lax.dynamic_slice_in_dim(pair, first_row, row_block, 0).astype(jnp.float32)
        pair_normed = normalize(pair_rows).astype(jnp.bfloat16)
        pair_bias = jnp.einsum('ikc,ch->hik', pair_normed.astype(jnp.float32), pair_proj.astype(jnp.float32)).astype(jnp.bfloat16)
        query_rows = lax.dynamic_slice_in_dim(queries, first_row, row_block, 0).astype(jnp.float32)
        query_rows = query_rows.reshape(row_block, H, head_dim)
        scores = jnp.einsum('qhd,khd->hqk', query_rows, key_heads) * score_scale + pair_bias.astype(jnp.float32)
        scores = jnp.where(key_live[None, None, :], scores, -1e+30)
        maxima = lax.optimization_barrier(jnp.max(scores, axis=-1, keepdims=True))
        weights = jnp.exp(scores - maxima)
        totals = lax.optimization_barrier(jnp.sum(weights, axis=-1))
        rounded = weights.astype(jnp.bfloat16)
        numerator = jnp.einsum('hqk,khd->qhd', rounded.astype(jnp.float32), value_heads)
        return numerator / jnp.transpose(totals)[:, :, None]
    averaged = lax.map(one_block, jnp.arange(block_count, dtype=jnp.int32)).reshape(TOKENS, features)
    attended = (gating * averaged).astype(jnp.bfloat16)
    return jnp.dot(attended, out_proj, preferred_element_type=jnp.float32).astype(jnp.bfloat16)
```

```python
import functools

import jax
import jax.numpy as jnp
from jax import lax
from jax.experimental import pallas as pl
from jax.experimental.pallas import tpu as pltpu
from jax.sharding import PartitionSpec as P

MESH = pl.DeviceIdType.MESH
F32, BF16 = jnp.float32, jnp.bfloat16


def normalize(matrix):
    average = jnp.mean(matrix, axis=-1, keepdims=True)
    centered = matrix - average
    variance = jnp.mean(centered * centered, axis=-1, keepdims=True)
    return centered * lax.rsqrt(variance + 1e-05)


def nt(a, b):
    return lax.dot_general(a, b, (((1,), (1,)), ((), ())), preferred_element_type=F32)


def kernel(
    nr, nc, chunks, group,
    singles, pair, chain, wproj, qbias, pproj, oproj, out,
    pair_v, w_v, o_v, rowbuf, keybuf, bias_s, q_s, k_s, v_s, part, recv,
    pair_sem, w_sem, row_send, row_recv, key_send, key_recv, out_send, out_recv,
):
    own, feats = singles.shape
    tile_rows, tile_cols, chans = pair.shape
    heads = pproj.shape[1]
    dim = feats // heads
    me_p, me_r, me_c = lax.axis_index("parts"), lax.axis_index("rows"), lax.axis_index("cols")
    flat = me_r * nc + me_c
    step = tile_rows // chunks

    def pair_copy(k):
        rows = pl.ds(k * step, step)
        return pltpu.make_async_copy(pair.at[rows], pair_v.at[rows], pair_sem.at[k])

    w_copy = pltpu.make_async_copy(wproj, w_v, w_sem.at[0])
    o_copy = pltpu.make_async_copy(oproj, o_v, w_sem.at[1])
    pair_copy(0).start()
    barrier = pltpu.get_barrier_semaphore()

    def greet(k, carry):
        other = lax.rem(flat + k, nr * nc)
        pl.semaphore_signal(
            barrier, inc=1, device_id=(me_p, other // nc, lax.rem(other, nc)), device_id_type=MESH
        )
        return carry

    lax.fori_loop(1, nr * nc, greet, 0)
    for k in range(1, chunks):
        pair_copy(k).start()
    w_copy.start()
    o_copy.start()

    wt = pproj[...].astype(F32).T.astype(BF16)

    def bias_chunk(k):
        pair_copy(k).wait()

        def body(g, carry):
            for u in range(group):
                i = k * step + g * group + u
                x = normalize(pair_v[i].astype(F32)).astype(BF16)
                bias_s[pl.ds(pl.multiple_of(i * heads, heads), heads), :] = nt(wt, x).astype(BF16)
            return carry

        lax.fori_loop(0, step // group, body, 0)

    bias_chunk(0)
    pl.semaphore_wait(barrier, nr * nc - 1)

    def row_copy(d):
        return pltpu.make_async_remote_copy(
            src_ref=singles, dst_ref=rowbuf.at[me_c],
            send_sem=row_send.at[d], recv_sem=row_recv.at[me_c],
            device_id=(me_p, me_r, lax.rem(me_c + d, nc)), device_id_type=MESH,
        )

    key_home = flat // nr
    key_slot = lax.rem(flat, nr)

    def key_copy(d):
        return pltpu.make_async_remote_copy(
            src_ref=singles, dst_ref=keybuf.at[key_slot],
            send_sem=key_send.at[d], recv_sem=key_recv.at[key_slot],
            device_id=(me_p, lax.rem(me_r + d, nr), key_home), device_id_type=MESH,
        )

    for d in range(1, nr):
        key_copy(d).start()

    @pl.when(key_home != me_c)
    def _():
        key_copy(0).start()

    for d in range(1, nc):
        row_copy(d).start()

    mine = singles[...]
    rowbuf[me_c] = mine

    @pl.when(key_home == me_c)
    def _():
        keybuf[key_slot] = mine

    for k in range(1, chunks):
        bias_chunk(k)

    w_copy.wait()
    o_copy.wait()
    normed = normalize(mine.astype(F32)).astype(BF16)
    gate_in = jnp.dot(normed, w_v[:, 3 * feats :], preferred_element_type=F32)
    gating = 1.0 / (1.0 + jnp.exp(-gate_in))

    for k in range(nr):
        @pl.when(me_c * nr + k != flat)
        def _():
            pltpu.make_async_remote_copy(
                src_ref=singles, dst_ref=keybuf.at[k],
                send_sem=key_send.at[0], recv_sem=key_recv.at[k],
                device_id=(me_p, me_r, lax.rem(me_c + 1, nc)), device_id_type=MESH,
            ).wait_recv()

    keys_in = keybuf[...].astype(F32).reshape(nr * own, feats)
    kn = normalize(keys_in).astype(BF16)
    kv = jnp.dot(kn, w_v[:, feats : 3 * feats], preferred_element_type=F32)
    k_s[...] = kv[:, :feats].astype(BF16)
    v_s[...] = kv[:, feats:].astype(BF16)

    def row_arrival(s):
        return pltpu.make_async_remote_copy(
            src_ref=singles, dst_ref=rowbuf.at[s],
            send_sem=row_send.at[0], recv_sem=row_recv.at[s],
            device_id=(me_p, me_r, lax.rem(me_c + 1, nc)), device_id_type=MESH,
        )

    for d in range(1, nc):
        row_arrival(lax.rem(me_c + d, nc)).wait_recv()
    rows_in = rowbuf[...].astype(F32).reshape(nc * own, feats)
    rn = normalize(rows_in).astype(BF16)
    q = jnp.dot(rn, w_v[:, :feats], preferred_element_type=F32) + qbias[...]
    q_s[...] = q.astype(BF16).astype(F32)

    live = chain[0]
    for k in range(1, chain.shape[0] - 1):
        live = live + chain[k]
    keys_at = lax.broadcasted_iota(jnp.int32, (1, tile_cols), 1) + me_c * tile_cols
    key_live = keys_at < live
    head_at = lax.broadcasted_iota(jnp.int32, (heads, feats), 0)
    feat_at = lax.broadcasted_iota(jnp.int32, (heads, feats), 1)
    block = (feat_at >= head_at * dim) & (feat_at < (head_at + 1) * dim)
    stat_head = lax.broadcasted_iota(jnp.int32, (heads, 128), 0)
    stat_lane = lax.broadcasted_iota(jnp.int32, (heads, 128), 1)
    scale = dim ** (-0.5)

    def attend(b, dst):
        qb = q_s[pl.ds(pl.multiple_of(b * own, own), own), :]
        qd = jnp.where(block[None], qb[:, None, :], 0.0).reshape(own * heads, feats).astype(BF16)
        bias = bias_s[pl.ds(pl.multiple_of(b * own * heads, own * heads), own * heads), :]
        s = nt(qd, k_s[...]) * scale + bias.astype(F32)
        s = jnp.where(key_live, s, -1e30)
        m = jnp.max(s, axis=-1, keepdims=True)
        p = jnp.exp(s - m)
        l = jnp.sum(p, axis=-1, keepdims=True)
        n = jnp.dot(p.astype(BF16), v_s[...], preferred_element_type=F32)
        n = jnp.sum(jnp.where(block[None], n.reshape(own, heads, feats), 0.0), axis=1)
        m3 = m.reshape(own, heads, 1)
        l3 = l.reshape(own, heads, 1)
        st = jnp.where((stat_lane == stat_head)[None], m3, 0.0)
        st = jnp.where((stat_lane == stat_head + 64)[None], l3, st)
        dst[:, :feats] = n
        dst[:, feats:] = jnp.sum(st, axis=1)

    def out_copy(d):
        to = lax.rem(me_c + d, nc)
        return pltpu.make_async_remote_copy(
            src_ref=part.at[to], dst_ref=recv.at[me_c],
            send_sem=out_send.at[d], recv_sem=out_recv.at[me_c],
            device_id=(me_p, me_r, to), device_id_type=MESH,
        )

    def remote_block(d, carry):
        to = lax.rem(me_c + d, nc)
        attend(to, part.at[to])
        out_copy(d).start()
        return carry

    lax.fori_loop(1, nc, remote_block, 0)
    attend(me_c, recv.at[me_c])

    for d in range(1, nc):
        s = lax.rem(me_c + d, nc)
        pltpu.make_async_remote_copy(
            src_ref=part.at[s], dst_ref=recv.at[s],
            send_sem=out_send.at[d], recv_sem=out_recv.at[s],
            device_id=(me_p, me_r, s), device_id_type=MESH,
        ).wait_recv()

    stats = recv[:, :, feats:]
    lanes = lax.broadcasted_iota(jnp.int32, (1, 1, 128), 2)
    top = jnp.max(stats, axis=0, keepdims=True)
    a = jnp.exp(stats - top)
    total = jnp.sum(a * pltpu.roll(stats, 64, 2), axis=0, keepdims=True)
    coef = jnp.where(lanes < heads, a / total, 0.0).reshape(nc * own, 128)
    eh = lax.broadcasted_iota(jnp.int32, (128, feats), 0)
    ef = lax.broadcasted_iota(jnp.int32, (128, feats), 1)
    expand = ((ef >= eh * dim) & (ef < (eh + 1) * dim)).astype(F32)
    wide = jnp.dot(coef, expand, precision=lax.Precision.HIGHEST, preferred_element_type=F32)
    averaged = jnp.sum(recv[:, :, :feats] * wide.reshape(nc, own, feats), axis=0)
    attended = (gating * averaged).astype(BF16)
    out[...] = jnp.dot(attended, o_v[...], preferred_element_type=F32).astype(out.dtype)

    for d in range(1, nr):
        key_copy(d).wait_send()

    @pl.when(key_home != me_c)
    def _():
        key_copy(0).wait_send()

    for d in range(1, nc):
        row_copy(d).wait_send()
        out_copy(d).wait_send()


def shards(nr, nc, singles, pair, chain_sizes, single_proj, query_bias, pair_proj, out_proj):
    own, feats = singles.shape
    tile_rows, tile_cols, chans = pair.shape
    heads = pair_proj.shape[1]
    chunks = 8
    vmem = pl.BlockSpec(memory_space=pltpu.VMEM)
    smem = pl.BlockSpec(memory_space=pltpu.SMEM)
    hbm = pl.BlockSpec(memory_space=pl.ANY)
    dma = pltpu.SemaphoreType.DMA
    return pl.pallas_call(
        functools.partial(kernel, nr, nc, chunks, 4),
        out_shape=jax.ShapeDtypeStruct((own, feats), BF16),
        in_specs=[vmem, hbm, smem, hbm, vmem, vmem, hbm],
        out_specs=vmem,
        scratch_shapes=[
            pltpu.VMEM(pair.shape, BF16),
            pltpu.VMEM(single_proj.shape, BF16),
            pltpu.VMEM(out_proj.shape, BF16),
            pltpu.VMEM((nc, own, feats), BF16),
            pltpu.VMEM((nr, own, feats), BF16),
            pltpu.VMEM((tile_rows * heads, tile_cols), BF16),
            pltpu.VMEM((tile_rows, feats), F32),
            pltpu.VMEM((tile_cols, feats), BF16),
            pltpu.VMEM((tile_cols, feats), BF16),
            pltpu.VMEM((nc, own, feats + 128), F32),
            pltpu.VMEM((nc, own, feats + 128), F32),
            dma((chunks,)), dma((2,)),
            dma((nc,)), dma((nc,)), dma((nr,)), dma((nr,)), dma((nc,)), dma((nc,)),
        ],
        compiler_params=pltpu.CompilerParams(
            collective_id=0, has_side_effects=True, vmem_limit_bytes=50 * 1024 * 1024
        ),
        name="pair_attention",
    )(singles, pair, chain_sizes, single_proj, query_bias.reshape(1, feats), pair_proj, out_proj)


def solution(mesh):
    placed = (
        P(("parts", "rows", "cols"), None),
        P(("parts", "rows"), "cols", None),
        P("parts"),
        P(),
        P(),
        P(),
        P(),
    )
    return jax.shard_map(
        functools.partial(shards, mesh.shape["rows"], mesh.shape["cols"]),
        mesh=mesh,
        in_specs=placed,
        out_specs=P(("parts", "rows", "cols"), None),
        check_vma=False,
    )
```

```python
import functools

import jax
import jax.numpy as jnp
from jax import lax
from jax.experimental import pallas as pl
from jax.experimental.pallas import tpu as pltpu
from jax.sharding import PartitionSpec as P

MESH = pl.DeviceIdType.MESH
F32, BF16 = jnp.float32, jnp.bfloat16


def normalize(matrix):
    average = jnp.mean(matrix, axis=-1, keepdims=True)
    centered = matrix - average
    variance = jnp.mean(centered * centered, axis=-1, keepdims=True)
    return centered * lax.rsqrt(variance + 1e-05)


def nt(a, b):
    return lax.dot_general(a, b, (((1,), (1,)), ((), ())), preferred_element_type=F32)


def kernel(
    nr, nc, chunks, group,
    singles_h, pair, chain_h, wproj, qbias_h, pproj_h, oproj, out,
    singles, chain, qbias, pproj, pair_v, w_v, o_v, rowbuf, keybuf, bias_s, q_s, k_s, v_s, wide_s, norm_s,
    part, part_stat, recv, recv_stat, pair_sem, w_sem,
    row_send, row_recv, key_send, key_recv, out_send, out_recv, stat_send, stat_recv,
):
    own, feats = singles.shape
    tile_rows, tile_cols, chans = pair.shape
    heads = pproj.shape[0]
    dim = feats // heads
    me_p, me_r, me_c = lax.axis_index("parts"), lax.axis_index("rows"), lax.axis_index("cols")
    flat = me_r * nc + me_c
    step = tile_rows // chunks

    def pair_copy(k):
        rows = pl.ds(k * step, step)
        return pltpu.make_async_copy(pair.at[rows], pair_v.at[rows], pair_sem.at[k])

    w_copy = pltpu.make_async_copy(wproj, w_v, w_sem.at[0])
    o_copy = pltpu.make_async_copy(oproj, o_v, w_sem.at[1])
    small = [
        pltpu.make_async_copy(src, dst, w_sem.at[2 + n])
        for n, (src, dst) in enumerate(
            ((singles_h, singles), (pproj_h, pproj), (chain_h, chain), (qbias_h, qbias))
        )
    ]
    small[0].start()
    small[1].start()
    pair_copy(0).start()
    barrier = pltpu.get_barrier_semaphore()

    def greet(k, carry):
        other = lax.rem(flat + k, nr * nc)
        pl.semaphore_signal(
            barrier, inc=1, device_id=(me_p, other // nc, lax.rem(other, nc)), device_id_type=MESH
        )
        return carry

    lax.fori_loop(1, nr * nc, greet, 0)
    for k in range(1, chunks):
        pair_copy(k).start()
    w_copy.start()
    small[2].start()
    small[3].start()
    o_copy.start()

    small[0].wait()
    small[1].wait()
    wt = pproj[...]
    tall = jnp.concatenate([wt] * step, axis=0)
    tall_at = lax.broadcasted_iota(jnp.int32, tall.shape, 0)
    for u in range(step):
        inside = (tall_at >= u * heads) & (tall_at < (u + 1) * heads)
        wide_s[:, u * chans : (u + 1) * chans] = jnp.where(inside, tall, 0).astype(BF16)

    def bias_chunk(k):
        pair_copy(k).wait()

        def body(g, carry):
            for u in range(group):
                i = g * group + u
                x = pair_v[k * step + i].astype(F32)
                x = normalize(x).astype(BF16)
                lanes_at = pl.ds(pl.multiple_of(i * chans, chans), chans)
                norm_s[pl.ds(k * tile_cols, tile_cols), lanes_at] = x
            return carry

        lax.fori_loop(0, step // group, body, 0)

    def bias_project(k):
        rows = norm_s[pl.ds(k * tile_cols, tile_cols), :]
        size = step * heads
        bias_s[pl.ds(k * size, size), :] = nt(rows, wide_s[...]).T.astype(BF16)

    bias_chunk(0)
    pl.semaphore_wait(barrier, nr * nc - 1)

    def row_copy(d):
        return pltpu.make_async_remote_copy(
            src_ref=singles, dst_ref=rowbuf.at[me_c],
            send_sem=row_send.at[d], recv_sem=row_recv.at[me_c],
            device_id=(me_p, me_r, lax.rem(me_c + d, nc)), device_id_type=MESH,
        )

    key_home = flat // nr
    key_slot = lax.rem(flat, nr)

    def key_copy(d):
        return pltpu.make_async_remote_copy(
            src_ref=singles, dst_ref=keybuf.at[key_slot],
            send_sem=key_send.at[d], recv_sem=key_recv.at[key_slot],
            device_id=(me_p, lax.rem(me_r + d, nr), key_home), device_id_type=MESH,
        )

    for d in range(1, nr):
        key_copy(d).start()

    @pl.when(key_home != me_c)
    def _():
        key_copy(0).start()

    for d in range(1, nc):
        row_copy(d).start()

    mine = singles[...]
    rowbuf[me_c] = mine

    @pl.when(key_home == me_c)
    def _():
        keybuf[key_slot] = mine

    def later_chunk(k, carry):
        bias_chunk(k)
        return carry

    lax.fori_loop(1, chunks, later_chunk, 0)

    def project_pair(k, carry):
        bias_project(2 * k)
        bias_project(2 * k + 1)
        return carry

    lax.fori_loop(0, chunks // 2, project_pair, 0)

    w_copy.wait()
    o_copy.wait()
    small[2].wait()
    small[3].wait()
    normed = normalize(mine.astype(F32)).astype(BF16)
    gate_in = jnp.dot(normed, w_v[:, 3 * feats :], preferred_element_type=F32)
    gating = 1.0 / (1.0 + jnp.exp(-gate_in))

    for k in range(nr):
        @pl.when(me_c * nr + k != flat)
        def _():
            pltpu.make_async_remote_copy(
                src_ref=singles, dst_ref=keybuf.at[k],
                send_sem=key_send.at[0], recv_sem=key_recv.at[k],
                device_id=(me_p, me_r, lax.rem(me_c + 1, nc)), device_id_type=MESH,
            ).wait_recv()

    keys_in = keybuf[...].astype(F32).reshape(nr * own, feats)
    kn = normalize(keys_in).astype(BF16)
    kv = jnp.dot(kn, w_v[:, feats : 3 * feats], preferred_element_type=F32)
    k_s[...] = kv[:, :feats].astype(BF16)
    values = kv[:, feats:].astype(BF16)
    v_s[:tile_cols, :] = values
    v_s[tile_cols:, :] = values

    def row_arrival(s):
        return pltpu.make_async_remote_copy(
            src_ref=singles, dst_ref=rowbuf.at[s],
            send_sem=row_send.at[0], recv_sem=row_recv.at[s],
            device_id=(me_p, me_r, lax.rem(me_c + 1, nc)), device_id_type=MESH,
        )

    for d in range(1, nc):
        row_arrival(lax.rem(me_c + d, nc)).wait_recv()
    rows_in = rowbuf[...].astype(F32).reshape(nc * own, feats)
    rn = normalize(rows_in).astype(BF16)
    q = jnp.dot(rn, w_v[:, :feats], preferred_element_type=F32) + qbias[...].reshape(1, feats)
    q_s[...] = q.astype(BF16).astype(F32)

    live = chain[0]
    for k in range(1, chain.shape[0] - 1):
        live = live + chain[k]
    keys_at = lax.broadcasted_iota(jnp.int32, (1, tile_cols), 1) + me_c * tile_cols
    key_live = keys_at < live
    head_at = lax.broadcasted_iota(jnp.int32, (heads, feats), 0)
    feat_at = lax.broadcasted_iota(jnp.int32, (heads, feats), 1)
    block = (feat_at >= head_at * dim) & (feat_at < (head_at + 1) * dim)
    stat_head = lax.broadcasted_iota(jnp.int32, (heads, 128), 0)
    stat_lane = lax.broadcasted_iota(jnp.int32, (heads, 128), 1)
    scale = dim ** (-0.5)

    def attend(b, dst, dst_stat):
        qb = q_s[pl.ds(pl.multiple_of(b * own, own), own), :]
        qd = jnp.where(block[None], qb[:, None, :], 0.0).reshape(own * heads, feats).astype(BF16)
        bias = bias_s[pl.ds(pl.multiple_of(b * own * heads, own * heads), own * heads), :]
        s = nt(qd, k_s[...]) * scale + bias.astype(F32)
        s = jnp.where(key_live, s, -1e30)
        m = jnp.max(s, axis=-1, keepdims=True)
        p = jnp.exp(s - m)
        l = jnp.sum(p, axis=-1, keepdims=True)
        high = p.astype(BF16)
        low = (p - high.astype(F32)).astype(BF16)
        p = jnp.concatenate([high, low], axis=1)
        n = jnp.dot(p, v_s[...], preferred_element_type=F32)
        n = jnp.sum(jnp.where(block[None], n.reshape(own, heads, feats), 0.0), axis=1)
        m3 = m.reshape(own, heads, 1)
        l3 = l.reshape(own, heads, 1)
        st = jnp.where((stat_lane == stat_head)[None], m3, 0.0)
        st = jnp.where((stat_lane == stat_head + 64)[None], l3, st)
        dst[...] = n.astype(BF16)
        dst_stat[...] = jnp.sum(st, axis=1)

    def out_copies(d, slot):
        to = lax.rem(me_c + d, nc)
        return [
            pltpu.make_async_remote_copy(
                src_ref=src.at[to], dst_ref=dst.at[slot],
                send_sem=send.at[d], recv_sem=arrive.at[slot],
                device_id=(me_p, me_r, to), device_id_type=MESH,
            )
            for src, dst, send, arrive in (
                (part, recv, out_send, out_recv),
                (part_stat, recv_stat, stat_send, stat_recv),
            )
        ]

    def remote_block(d, carry):
        to = lax.rem(me_c + d, nc)
        attend(to, part.at[to], part_stat.at[to])
        for copy in out_copies(d, me_c):
            copy.start()
        return carry

    lax.fori_loop(1, nc, remote_block, 0)
    attend(me_c, recv.at[me_c], recv_stat.at[me_c])

    for d in range(1, nc):
        for copy in out_copies(d, lax.rem(me_c + d, nc)):
            copy.wait_recv()

    stats = recv_stat[...]
    lanes = lax.broadcasted_iota(jnp.int32, (1, 1, 128), 2)
    top = jnp.max(stats, axis=0, keepdims=True)
    a = jnp.exp(stats - top)
    total = jnp.sum(a * pltpu.roll(stats, 64, 2), axis=0, keepdims=True)
    coef = jnp.where(lanes < heads, a / total, 0.0).reshape(nc * own, 128)
    eh = lax.broadcasted_iota(jnp.int32, (128, feats), 0)
    ef = lax.broadcasted_iota(jnp.int32, (128, feats), 1)
    expand = ((ef >= eh * dim) & (ef < (eh + 1) * dim)).astype(F32)
    wide = jnp.dot(coef, expand, precision=lax.Precision.HIGHEST, preferred_element_type=F32)
    averaged = jnp.sum(recv[...].astype(F32) * wide.reshape(nc, own, feats), axis=0)
    attended = (gating * averaged).astype(BF16)
    out[...] = jnp.dot(attended, o_v[...], preferred_element_type=F32).astype(out.dtype)

    for d in range(1, nr):
        key_copy(d).wait_send()

    @pl.when(key_home != me_c)
    def _():
        key_copy(0).wait_send()

    for d in range(1, nc):
        row_copy(d).wait_send()
        for copy in out_copies(d, me_c):
            copy.wait_send()


def shards(nr, nc, singles, pair, chain_sizes, single_proj, query_bias, pair_proj, out_proj):
    own, feats = singles.shape
    tile_rows, tile_cols, chans = pair.shape
    heads = pair_proj.shape[1]
    chunks = 8
    vmem = pl.BlockSpec(memory_space=pltpu.VMEM)
    hbm = pl.BlockSpec(memory_space=pltpu.HBM)
    dma = pltpu.SemaphoreType.DMA
    return pl.pallas_call(
        functools.partial(kernel, nr, nc, chunks, 4),
        out_shape=jax.ShapeDtypeStruct((own, feats), BF16),
        in_specs=[hbm] * 7,
        out_specs=vmem,
        scratch_shapes=[
            pltpu.VMEM(singles.shape, BF16),
            pltpu.SMEM(chain_sizes.shape, jnp.int32),
            pltpu.VMEM(query_bias.shape, F32),
            pltpu.VMEM((heads, chans), BF16),
            pltpu.VMEM(pair.shape, BF16),
            pltpu.VMEM(single_proj.shape, BF16),
            pltpu.VMEM(out_proj.shape, BF16),
            pltpu.VMEM((nc, own, feats), BF16),
            pltpu.VMEM((nr, own, feats), BF16),
            pltpu.VMEM((tile_rows * heads, tile_cols), BF16),
            pltpu.VMEM((tile_rows, feats), F32),
            pltpu.VMEM((tile_cols, feats), BF16),
            pltpu.VMEM((2 * tile_cols, feats), BF16),
            pltpu.VMEM((tile_rows // chunks * heads, tile_rows // chunks * chans), BF16),
            pltpu.VMEM((chunks * tile_cols, tile_rows // chunks * chans), BF16),
            pltpu.VMEM((nc, own, feats), BF16),
            pltpu.VMEM((nc, own, 128), F32),
            pltpu.VMEM((nc, own, feats), BF16),
            pltpu.VMEM((nc, own, 128), F32),
            dma((chunks,)), dma((6,)),
            dma((nc,)), dma((nc,)), dma((nr,)), dma((nr,)),
            dma((nc,)), dma((nc,)), dma((nc,)), dma((nc,)),
        ],
        compiler_params=pltpu.CompilerParams(
            collective_id=0, has_side_effects=True
        ),
        name="pair_attention",
    )(singles, pair, chain_sizes, single_proj, query_bias, pair_proj.T, out_proj)


def solution(mesh):
    placed = (
        P(("parts", "rows", "cols"), None),
        P(("parts", "rows"), "cols", None),
        P("parts"),
        P(),
        P(),
        P(),
        P(),
    )
    return jax.shard_map(
        functools.partial(shards, mesh.shape["rows"], mesh.shape["cols"]),
        mesh=mesh,
        in_specs=placed,
        out_specs=P(("parts", "rows", "cols"), None),
        check_vma=False,
    )
```

```python
import functools

import jax
import jax.numpy as jnp
from jax import lax
from jax.experimental import pallas as pl
from jax.experimental.pallas import tpu as pltpu
from jax.sharding import PartitionSpec as P

MESH = pl.DeviceIdType.MESH
F32, BF16 = jnp.float32, jnp.bfloat16


def normalize(matrix):
    average = jnp.mean(matrix, axis=-1, keepdims=True)
    centered = matrix - average
    variance = jnp.mean(centered * centered, axis=-1, keepdims=True)
    return centered * lax.rsqrt(variance + 1e-05)


def nt(a, b):
    return lax.dot_general(a, b, (((1,), (1,)), ((), ())), preferred_element_type=F32)


def kernel(
    nr, nc, chunks, group,
    singles_h, pair, chain_h, wproj, qbias_h, pproj_h, oproj, out,
    singles, chain, qbias, pproj, pair_v, w_v, o_v, rowbuf, keybuf, bias_s, q_s, k_s, v_s, wide_s, norm_s,
    part, part_stat, recv, recv_stat, pair_sem, w_sem,
    row_send, row_recv, key_send, key_recv, out_send, out_recv, stat_send, stat_recv,
):
    own, feats = singles.shape
    tile_rows, tile_cols, chans = pair.shape
    heads = pproj.shape[0]
    dim = feats // heads
    me_p, me_r, me_c = lax.axis_index("parts"), lax.axis_index("rows"), lax.axis_index("cols")
    flat = me_r * nc + me_c
    step = tile_rows // chunks

    def pair_copy(k):
        rows = pl.ds(k * step, step)
        return pltpu.make_async_copy(pair.at[rows], pair_v.at[rows], pair_sem.at[k])

    w_copy = pltpu.make_async_copy(wproj, w_v, w_sem.at[0])
    o_copy = pltpu.make_async_copy(oproj, o_v, w_sem.at[1])
    small = [
        pltpu.make_async_copy(src, dst, w_sem.at[2 + n])
        for n, (src, dst) in enumerate(
            ((singles_h, singles), (pproj_h, pproj), (chain_h, chain), (qbias_h, qbias))
        )
    ]
    small[0].start()
    small[1].start()
    pair_copy(0).start()
    barrier = pltpu.get_barrier_semaphore()

    def greet(k, carry):
        other = lax.rem(flat + k, nr * nc)
        pl.semaphore_signal(
            barrier, inc=1, device_id=(me_p, other // nc, lax.rem(other, nc)), device_id_type=MESH
        )
        return carry

    lax.fori_loop(1, nr * nc, greet, 0)
    for k in range(1, chunks):
        pair_copy(k).start()
    w_copy.start()
    small[2].start()
    small[3].start()
    o_copy.start()

    small[0].wait()
    small[1].wait()
    wt = pproj[...]
    tall = jnp.concatenate([wt] * step, axis=0)
    tall_at = lax.broadcasted_iota(jnp.int32, tall.shape, 0)
    for u in range(step):
        inside = (tall_at >= u * heads) & (tall_at < (u + 1) * heads)
        wide_s[:, u * chans : (u + 1) * chans] = jnp.where(inside, tall, 0).astype(BF16)

    def bias_chunk(k):
        pair_copy(k).wait()

        def body(g, carry):
            for u in range(group):
                i = g * group + u
                x = pair_v[k * step + i].astype(F32)
                x = normalize(x).astype(BF16)
                lanes_at = pl.ds(pl.multiple_of(i * chans, chans), chans)
                norm_s[pl.ds(k * tile_cols, tile_cols), lanes_at] = x
            return carry

        lax.fori_loop(0, step // group, body, 0)

    batch = chunks // 2

    def bias_project(g, carry):
        rows = norm_s[pl.ds(g * batch * tile_cols, batch * tile_cols), :]
        size = step * heads
        wide_bias = nt(rows, wide_s[...])
        for u in range(batch):
            piece = wide_bias[u * tile_cols : (u + 1) * tile_cols, :]
            bias_s[pl.ds((g * batch + u) * size, size), :] = piece.T.astype(BF16)
        return carry

    def later_chunk(k, carry):
        bias_chunk(k)
        return carry

    early = min(3, chunks)
    lax.fori_loop(0, early, later_chunk, 0)
    pl.semaphore_wait(barrier, nr * nc - 1)

    def row_copy(d):
        return pltpu.make_async_remote_copy(
            src_ref=singles, dst_ref=rowbuf.at[me_c],
            send_sem=row_send.at[d], recv_sem=row_recv.at[me_c],
            device_id=(me_p, me_r, lax.rem(me_c + d, nc)), device_id_type=MESH,
        )

    key_home = flat // nr
    key_slot = lax.rem(flat, nr)

    def key_copy(d):
        return pltpu.make_async_remote_copy(
            src_ref=singles, dst_ref=keybuf.at[key_slot],
            send_sem=key_send.at[d], recv_sem=key_recv.at[key_slot],
            device_id=(me_p, lax.rem(me_r + d, nr), key_home), device_id_type=MESH,
        )

    for d in range(1, nr):
        key_copy(d).start()

    @pl.when(key_home != me_c)
    def _():
        key_copy(0).start()

    for d in range(1, nc):
        row_copy(d).start()

    mine = singles[...]
    rowbuf[me_c] = mine

    @pl.when(key_home == me_c)
    def _():
        keybuf[key_slot] = mine

    lax.fori_loop(early, chunks, later_chunk, 0)

    lax.fori_loop(0, chunks // batch, bias_project, 0)

    w_copy.wait()
    o_copy.wait()
    small[2].wait()
    small[3].wait()
    normed = normalize(mine.astype(F32)).astype(BF16)
    gate_in = jnp.dot(normed, w_v[:, 3 * feats :], preferred_element_type=F32)
    gating = 1.0 / (1.0 + jnp.exp(-gate_in))

    for k in range(nr):
        @pl.when(me_c * nr + k != flat)
        def _():
            pltpu.make_async_remote_copy(
                src_ref=singles, dst_ref=keybuf.at[k],
                send_sem=key_send.at[0], recv_sem=key_recv.at[k],
                device_id=(me_p, me_r, lax.rem(me_c + 1, nc)), device_id_type=MESH,
            ).wait_recv()

    keys_in = keybuf[...].astype(F32).reshape(nr * own, feats)
    kn = normalize(keys_in).astype(BF16)
    kv = jnp.dot(kn, w_v[:, feats : 3 * feats], preferred_element_type=F32)
    k_s[...] = kv[:, :feats].astype(BF16)
    values = kv[:, feats:].astype(BF16)
    v_s[:tile_cols, :] = values
    v_s[tile_cols:, :] = values

    def row_arrival(s):
        return pltpu.make_async_remote_copy(
            src_ref=singles, dst_ref=rowbuf.at[s],
            send_sem=row_send.at[0], recv_sem=row_recv.at[s],
            device_id=(me_p, me_r, lax.rem(me_c + 1, nc)), device_id_type=MESH,
        )

    for d in range(1, nc):
        row_arrival(lax.rem(me_c + d, nc)).wait_recv()
    rows_in = rowbuf[...].astype(F32).reshape(nc * own, feats)
    rn = normalize(rows_in).astype(BF16)
    q = jnp.dot(rn, w_v[:, :feats], preferred_element_type=F32) + qbias[...].reshape(1, feats)
    q_s[...] = q.astype(BF16).astype(F32)

    live = chain[0]
    for k in range(1, chain.shape[0] - 1):
        live = live + chain[k]
    keys_at = lax.broadcasted_iota(jnp.int32, (1, tile_cols), 1) + me_c * tile_cols
    key_live = keys_at < live
    head_at = lax.broadcasted_iota(jnp.int32, (heads, feats), 0)
    feat_at = lax.broadcasted_iota(jnp.int32, (heads, feats), 1)
    block = (feat_at >= head_at * dim) & (feat_at < (head_at + 1) * dim)
    stat_head = lax.broadcasted_iota(jnp.int32, (heads, 128), 0)
    stat_lane = lax.broadcasted_iota(jnp.int32, (heads, 128), 1)
    scale = dim ** (-0.5)

    def attend(b, dst, dst_stat):
        qb = q_s[pl.ds(pl.multiple_of(b * own, own), own), :]
        qd = jnp.where(block[None], qb[:, None, :], 0.0).reshape(own * heads, feats).astype(BF16)
        bias = bias_s[pl.ds(pl.multiple_of(b * own * heads, own * heads), own * heads), :]
        s = nt(qd, k_s[...]) * scale + bias.astype(F32)
        s = jnp.where(key_live, s, -1e30)
        m = jnp.max(s, axis=-1, keepdims=True)
        p = jnp.exp(s - m)
        l = jnp.sum(p, axis=-1, keepdims=True)
        high = p.astype(BF16)
        low = (p - high.astype(F32)).astype(BF16)
        p = jnp.concatenate([high, low], axis=1)
        n = jnp.dot(p, v_s[...], preferred_element_type=F32)
        n = jnp.sum(jnp.where(block[None], n.reshape(own, heads, feats), 0.0), axis=1)
        m3 = m.reshape(own, heads, 1)
        l3 = l.reshape(own, heads, 1)
        st = jnp.where((stat_lane == stat_head)[None], m3, 0.0)
        st = jnp.where((stat_lane == stat_head + 64)[None], l3, st)
        dst[...] = n.astype(BF16)
        dst_stat[...] = jnp.sum(st, axis=1)

    def out_copies(d, slot):
        to = lax.rem(me_c + d, nc)
        return [
            pltpu.make_async_remote_copy(
                src_ref=src.at[to], dst_ref=dst.at[slot],
                send_sem=send.at[d], recv_sem=arrive.at[slot],
                device_id=(me_p, me_r, to), device_id_type=MESH,
            )
            for src, dst, send, arrive in (
                (part, recv, out_send, out_recv),
                (part_stat, recv_stat, stat_send, stat_recv),
            )
        ]

    def remote_block(d, carry):
        to = lax.rem(me_c + d, nc)
        attend(to, part.at[to], part_stat.at[to])
        for copy in out_copies(d, me_c):
            copy.start()
        return carry

    lax.fori_loop(1, nc, remote_block, 0)
    attend(me_c, recv.at[me_c], recv_stat.at[me_c])

    for d in range(1, nc):
        for copy in out_copies(d, lax.rem(me_c + d, nc)):
            copy.wait_recv()

    stats = recv_stat[...]
    lanes = lax.broadcasted_iota(jnp.int32, (1, 1, 128), 2)
    top = jnp.max(stats, axis=0, keepdims=True)
    a = jnp.exp(stats - top)
    total = jnp.sum(a * pltpu.roll(stats, 64, 2), axis=0, keepdims=True)
    coef = jnp.where(lanes < heads, a / total, 0.0).reshape(nc * own, 128)
    eh = lax.broadcasted_iota(jnp.int32, (128, feats), 0)
    ef = lax.broadcasted_iota(jnp.int32, (128, feats), 1)
    expand = ((ef >= eh * dim) & (ef < (eh + 1) * dim)).astype(F32)
    wide = jnp.dot(coef, expand, precision=lax.Precision.HIGHEST, preferred_element_type=F32)
    averaged = jnp.sum(recv[...].astype(F32) * wide.reshape(nc, own, feats), axis=0)
    attended = (gating * averaged).astype(BF16)
    out[...] = jnp.dot(attended, o_v[...], preferred_element_type=F32).astype(out.dtype)

    for d in range(1, nr):
        key_copy(d).wait_send()

    @pl.when(key_home != me_c)
    def _():
        key_copy(0).wait_send()

    for d in range(1, nc):
        row_copy(d).wait_send()
        for copy in out_copies(d, me_c):
            copy.wait_send()


def shards(nr, nc, singles, pair, chain_sizes, single_proj, query_bias, pair_proj, out_proj):
    own, feats = singles.shape
    tile_rows, tile_cols, chans = pair.shape
    heads = pair_proj.shape[1]
    chunks = 8
    vmem = pl.BlockSpec(memory_space=pltpu.VMEM)
    hbm = pl.BlockSpec(memory_space=pltpu.HBM)
    dma = pltpu.SemaphoreType.DMA
    return pl.pallas_call(
        functools.partial(kernel, nr, nc, chunks, 4),
        out_shape=jax.ShapeDtypeStruct((own, feats), BF16),
        in_specs=[hbm] * 7,
        out_specs=vmem,
        scratch_shapes=[
            pltpu.VMEM(singles.shape, BF16),
            pltpu.SMEM(chain_sizes.shape, jnp.int32),
            pltpu.VMEM(query_bias.shape, F32),
            pltpu.VMEM((heads, chans), BF16),
            pltpu.VMEM(pair.shape, BF16),
            pltpu.VMEM(single_proj.shape, BF16),
            pltpu.VMEM(out_proj.shape, BF16),
            pltpu.VMEM((nc, own, feats), BF16),
            pltpu.VMEM((nr, own, feats), BF16),
            pltpu.VMEM((tile_rows * heads, tile_cols), BF16),
            pltpu.VMEM((tile_rows, feats), F32),
            pltpu.VMEM((tile_cols, feats), BF16),
            pltpu.VMEM((2 * tile_cols, feats), BF16),
            pltpu.VMEM((tile_rows // chunks * heads, tile_rows // chunks * chans), BF16),
            pltpu.VMEM((chunks * tile_cols, tile_rows // chunks * chans), BF16),
            pltpu.VMEM((nc, own, feats), BF16),
            pltpu.VMEM((nc, own, 128), F32),
            pltpu.VMEM((nc, own, feats), BF16),
            pltpu.VMEM((nc, own, 128), F32),
            dma((chunks,)), dma((6,)),
            dma((nc,)), dma((nc,)), dma((nr,)), dma((nr,)),
            dma((nc,)), dma((nc,)), dma((nc,)), dma((nc,)),
        ],
        compiler_params=pltpu.CompilerParams(
            collective_id=0, has_side_effects=True
        ),
        name="pair_attention",
    )(singles, pair, chain_sizes, single_proj, query_bias, pair_proj.T, out_proj)


def solution(mesh):
    placed = (
        P(("parts", "rows", "cols"), None),
        P(("parts", "rows"), "cols", None),
        P("parts"),
        P(),
        P(),
        P(),
        P(),
    )
    return jax.shard_map(
        functools.partial(shards, mesh.shape["rows"], mesh.shape["cols"]),
        mesh=mesh,
        in_specs=placed,
        out_specs=P(("parts", "rows", "cols"), None),
        check_vma=False,
    )
```
